32 devices in a mesh: row: 2 (over core), sa: 16 (over z, y, x).
Axes of the slice: x: 2, y: 2, z: 4, core: 2. Of those that a mesh axis runs over, the one named last changes fastest.
Arguments:
- rep_w1: float32 [4, 2, 64, 4096], P('row', None, None, 'sa'), may hold values from -6 to 6
- rep_w3: float32 [4, 2, 64, 4096], P('row', None, None, 'sa'), may hold values from -6 to 6
- rep_w2: float32 [4, 2, 64, 4096], P('row', None, None, 'sa'), may hold values from -6 to 6
- rep_gate: float32 [4, 2, 4096], P('row', None, 'sa'), may hold values from -6 to 6
Outputs:
- serve_w1: bfloat16 [2, 64, 4096], P('row', 'sa')
- serve_w3: bfloat16 [2, 64, 4096], P('row', 'sa')
- serve_w2: bfloat16 [2, 64, 4096], P('row', 'sa')
- serve_gate: bfloat16 [2, 4096], replicated
- soup_norms: float32 [2, 4], P('row')
- replica_norms: float32 [4, 2, 4], P('row')
The draws below stay inside these ranges and needn't reach their ends.
All inputs are finite; a program needn't handle non-finite values.
Results may differ from the reference program's by a relative error of at most 0.001.
Values may be sent and summed in bfloat16 or wider, within the bound.
A program may use at most 64 MiB of HBM per device.

```python
import jax
import jax.numpy as jnp
from jax import lax

D = 4096
EXPERTS = 2
REPLICAS = 4
HID = 64


def raised(drawn, key, source, target, blocks, factor):
    def block_of(axis_at):
        return (jnp.arange(drawn.shape[axis_at]) // (drawn.shape[axis_at] // blocks)).reshape((-1,) + (1,) * (drawn.ndim - 1 - axis_at))

    first = jax.random.permutation(key, blocks)[block_of(target)]
    other_side = (block_of(target) + blocks // 2) % blocks
    return jnp.where((block_of(source) == first) | (block_of(source) == other_side), factor * drawn, drawn)


def block_scale(stream_key, shape, cuts, low, largest):
    def one(axis_at, blocks):
        draws = jax.random.uniform(jax.random.fold_in(jax.random.fold_in(stream_key, 6), axis_at), (blocks,), jnp.float32, low / len(cuts), largest / len(cuts))
        return jnp.repeat(jnp.exp(draws), shape[axis_at] // blocks).reshape((-1,) + (1,) * (len(shape) - axis_at - 1))

    factor_of = one(*cuts[0])
    for cut in cuts[1:]:
        factor_of = factor_of * one(*cut)
    return factor_of


def heavy_noise(own_key, dims, width, limit, shards, heavy, dtype=jnp.bfloat16):
    drawn = width * jax.random.normal(own_key, dims, jnp.float32)
    if shards:
        drawn = drawn * block_scale(own_key, dims, shards, -0.22, 0.18)
    return jnp.clip(raised(drawn, jax.random.fold_in(own_key, 3), *heavy), -limit, limit).astype(dtype)


def setup_inputs(seed: int = 0) -> dict:
    streams_of = jax.random.split(jax.random.key(seed), 5)
    rep_w1 = heavy_noise(streams_of[0], (REPLICAS, EXPERTS, HID, D), 1.0, 6.0, ((0, 2), (3, 16)), (3, 0, 4, 2.0), jnp.float32)
    rep_w3 = heavy_noise(streams_of[1], (REPLICAS, EXPERTS, HID, D), 1.0, 6.0, ((0, 2), (3, 16)), (3, 0, 4, 2.0), jnp.float32)
    rep_w2 = heavy_noise(streams_of[2], (REPLICAS, EXPERTS, HID, D), 1.0, 6.0, ((0, 2), (3, 16)), (3, 0, 4, 2.0), jnp.float32)
    rep_gate = heavy_noise(streams_of[3], (REPLICAS, EXPERTS, D), 1.0, 6.0, ((0, 2), (2, 16)), (2, 0, 4, 2.0), jnp.float32)
    return {"rep_w1": rep_w1, "rep_w3": rep_w3, "rep_w2": rep_w2, "rep_gate": rep_gate}


def square_sums(values, dims_summed):
    return lax.optimization_barrier(jnp.sum(values * values, axis=dims_summed))

def reference(rep_w1, rep_w3, rep_w2, rep_gate):
    weights = (rep_w1, rep_w3, rep_w2)
    served_list = []
    for weight in weights:
        soup = lax.optimization_barrier(jnp.sum(weight, axis=0)) / REPLICAS
        served_list.append(soup.astype(jnp.bfloat16))
    gate_soup = lax.optimization_barrier(jnp.sum(rep_gate, axis=0)) / REPLICAS
    serve_gate = gate_soup.astype(jnp.bfloat16)
    expert_entries = HID * D
    soup_columns = [jnp.sqrt(square_sums(served.astype(jnp.float32), (1, 2)) / expert_entries) for served in served_list]
    soup_columns.append(jnp.sqrt(square_sums(serve_gate.astype(jnp.float32), 1) / D))
    soup_norms = jnp.stack(soup_columns, axis=1)
    replica_columns = [jnp.sqrt(square_sums(weight, (2, 3)) / expert_entries) for weight in weights]
    replica_columns.append(jnp.sqrt(square_sums(rep_gate, 2) / D))
    replica_norms = jnp.stack(replica_columns, axis=2)
    return (served_list[0], served_list[1], served_list[2], serve_gate, soup_norms, replica_norms)
```

```python
import functools

import jax
import jax.numpy as jnp
from jax import lax
from jax.experimental import pallas as pl
from jax.experimental.pallas import tpu as pltpu
from jax.sharding import PartitionSpec as P

MESH = pl.DeviceIdType.MESH
F32 = jnp.float32
BF16 = jnp.bfloat16


def scaled(total, replicas):
    if replicas & (replicas - 1) == 0:
        return total * (1.0 / replicas)
    return total / replicas


def square_sum(values):
    squares = values * values
    while squares.ndim > 2:
        squares = jnp.sum(squares, axis=0)
    rows = jnp.sum(squares, axis=0, keepdims=True)
    return jnp.sum(rows, axis=1, keepdims=True)


def kernel(
    rows, n, replicas, counts,
    w1_hbm, w3_hbm, w2_hbm, gate_hbm,
    out1, out3, out2, gate_out, soup_out, rep_out,
    w_in, gate_in, part, part_got, gate_slots, block, gate_block, stats_send, stats_slots,
    in_sem, row_send, row_recv, gate_row_send, gate_row_recv, sa_send, sa_recv,
):
    sources = (w1_hbm, w3_hbm, w2_hbm)
    outs = (out1, out3, out2)
    held, experts, hidden, width = w1_hbm.shape
    own_experts = experts // rows
    own_hidden = hidden // n
    row = lax.axis_index("row")
    me = lax.axis_index("sa")

    loads = [pltpu.make_async_copy(gate_hbm, gate_in, in_sem.at[3])]
    loads += [pltpu.make_async_copy(sources[t], w_in.at[t], in_sem.at[t]) for t in range(3)]
    for load in loads:
        load.start()

    barrier = pltpu.get_barrier_semaphore()

    def greet(step, carry):
        pl.semaphore_signal(
            barrier, inc=1, device_id={"sa": lax.rem(me + step, n)}, device_id_type=MESH
        )
        return carry

    for step in range(1, rows):
        pl.semaphore_signal(
            barrier, inc=1, device_id={"row": lax.rem(row + step, rows)}, device_id_type=MESH
        )
    lax.fori_loop(1, n, greet, 0)

    lane = lax.broadcasted_iota(jnp.int32, (1, stats_send.shape[1]), 1)
    stats = jnp.zeros((1, stats_send.shape[1]), F32)
    soup_lanes = 4 * own_experts

    def rep_lane(replica, expert, t):
        return soup_lanes + 4 * (replica * experts + expert) + t

    loads[0].wait()
    gate_sum = gate_in[0]
    for replica in range(1, held):
        gate_sum = gate_sum + gate_in[replica]
    gate_slots[row] = gate_sum
    for t in range(3):
        loads[1 + t].wait()
        for step in range(1, rows):
            first = lax.rem(row + step, rows) * own_experts
            total = w_in[t, 0, pl.ds(first, own_experts)]
            for replica in range(1, held):
                total = total + w_in[t, replica, pl.ds(first, own_experts)]
            part[t, step - 1] = total

    pl.semaphore_wait(barrier, rows - 1 + n - 1)

    gate_copies = []
    part_copies = []
    for step in range(1, rows):
        gate_copies.append(
            pltpu.make_async_remote_copy(
                src_ref=gate_slots.at[row],
                dst_ref=gate_slots.at[row],
                send_sem=gate_row_send.at[step - 1],
                recv_sem=gate_row_recv.at[step - 1],
                device_id={"row": lax.rem(row + step, rows)},
                device_id_type=MESH,
            )
        )
        gate_copies[-1].start()
    for t in range(3):
        for step in range(1, rows):
            part_copies.append(
                pltpu.make_async_remote_copy(
                    src_ref=part.at[t, step - 1],
                    dst_ref=part_got.at[t, step - 1],
                    send_sem=row_send.at[t, step - 1],
                    recv_sem=row_recv.at[t, step - 1],
                    device_id={"row": lax.rem(row + step, rows)},
                    device_id_type=MESH,
                )
            )
            part_copies[-1].start()

    for replica in range(held):
        for expert in range(experts):
            for t in range(3):
                stats = jnp.where(
                    lane == rep_lane(replica, expert, t),
                    square_sum(w_in[t, replica, expert]),
                    stats,
                )
            stats = jnp.where(
                lane == rep_lane(replica, expert, 3),
                square_sum(gate_in[replica, pl.ds(expert, 1)]),
                stats,
            )

    columns = pl.ds(pl.multiple_of(me * width, width), width)
    own_first = row * own_experts

    for copy in gate_copies:
        copy.wait_recv()
    gate_total = gate_slots[0]
    for other in range(1, rows):
        gate_total = gate_total + gate_slots[other]
    served_gate = scaled(gate_total, replicas).astype(BF16)
    gate_block[...] = served_gate
    gate_out[:, columns] = served_gate

    def send_gate(step, carry):
        pltpu.make_async_remote_copy(
            src_ref=gate_block,
            dst_ref=gate_out.at[:, columns],
            send_sem=sa_send.at[3],
            recv_sem=sa_recv.at[3],
            device_id={"sa": lax.rem(me + step, n)},
            device_id_type=MESH,
        ).start()
        return carry

    lax.fori_loop(1, n, send_gate, 0)

    gate_wide = served_gate.astype(F32)
    gate_squares = jnp.sum(gate_wide * gate_wide, axis=1, keepdims=True)
    expert_row = lax.broadcasted_iota(jnp.int32, gate_squares.shape, 0)
    for own in range(own_experts):
        square = jnp.sum(
            jnp.where(expert_row == own_first + own, gate_squares, 0.0), axis=0, keepdims=True
        )
        stats = jnp.where(lane == 4 * own + 3, square, stats)

    for t in range(3):
        for copy in part_copies[t * (rows - 1):(t + 1) * (rows - 1)]:
            copy.wait_recv()
        total = w_in[t, 0, pl.ds(own_first, own_experts)]
        for replica in range(1, held):
            total = total + w_in[t, replica, pl.ds(own_first, own_experts)]
        for step in range(1, rows):
            total = total + part_got[t, step - 1]
        served = scaled(total, replicas).astype(BF16)
        for dest in range(n):
            block[t, dest] = served[:, dest * own_hidden:(dest + 1) * own_hidden]

        def send_block(step, carry, t=t):
            peer = lax.rem(me + step, n)
            pltpu.make_async_remote_copy(
                src_ref=block.at[t, peer],
                dst_ref=outs[t].at[:, :, columns],
                send_sem=sa_send.at[t],
                recv_sem=sa_recv.at[t],
                device_id={"sa": peer},
                device_id_type=MESH,
            ).start()
            return carry

        lax.fori_loop(1, n, send_block, 0)
        outs[t][:, :, columns] = block[t, me]
        for own in range(own_experts):
            stats = jnp.where(
                lane == 4 * own + t, square_sum(served[own].astype(F32)), stats
            )

    stats_send[...] = stats
    stats_slots[me] = stats

    def send_stats(step, carry):
        pltpu.make_async_remote_copy(
            src_ref=stats_send,
            dst_ref=stats_slots.at[me],
            send_sem=sa_send.at[4],
            recv_sem=sa_recv.at[4],
            device_id={"sa": lax.rem(me + step, n)},
            device_id_type=MESH,
        ).start()
        return carry

    lax.fori_loop(1, n, send_stats, 0)

    others = pl.ds(0, (n - 1) * width)
    landed = [outs[t].at[:, :, others] for t in range(3)]
    landed += [gate_out.at[:, others], stats_slots.at[pl.ds(0, n - 1)]]
    pltpu.make_async_copy(landed[4], landed[4], sa_recv.at[4]).wait()
    norms = stats_slots[0]
    for source in range(1, n):
        norms = norms + stats_slots[source]
    norms = jnp.sqrt(jnp.where(lane % 4 == 3, norms / counts[1], norms / counts[0]))
    for own in range(own_experts):
        soup_out[pl.ds(own, 1), :] = norms[:, 4 * own:4 * own + 4]
    for replica in range(held):
        for expert in range(experts):
            at = rep_lane(replica, expert, 0)
            rep_out[replica, pl.ds(expert, 1), :] = norms[:, at:at + 4]

    for t in (3, 0, 1, 2):
        pltpu.make_async_copy(landed[t], landed[t], sa_recv.at[t]).wait()
    for copy in gate_copies + part_copies:
        copy.wait_send()
    for t in range(5):
        pltpu.make_async_copy(landed[t], landed[t], sa_send.at[t]).wait()


def local(rep_w1, rep_w3, rep_w2, rep_gate, rows, n):
    held, experts, hidden, width = rep_w1.shape
    own_experts, own_hidden = experts // rows, hidden // n
    lanes = -(-4 * (own_experts + held * experts) // 128) * 128
    vmem = pl.BlockSpec(memory_space=pltpu.VMEM)
    served = jax.ShapeDtypeStruct((own_experts, own_hidden, n * width), BF16)
    return pl.pallas_call(
        functools.partial(
            kernel, rows, n, held * rows, (float(hidden * width * n), float(width * n))
        ),
        out_shape=(
            served,
            served,
            served,
            jax.ShapeDtypeStruct((experts, n * width), BF16),
            jax.ShapeDtypeStruct((own_experts, 4), F32),
            jax.ShapeDtypeStruct((held, experts, 4), F32),
        ),
        in_specs=[pl.BlockSpec(memory_space=pl.ANY)] * 4,
        out_specs=(vmem,) * 6,
        scratch_shapes=[
            pltpu.VMEM((3, held, experts, hidden, width), F32),
            pltpu.VMEM((held, experts, width), F32),
            pltpu.VMEM((3, rows - 1, own_experts, hidden, width), F32),
            pltpu.VMEM((3, rows - 1, own_experts, hidden, width), F32),
            pltpu.VMEM((rows, experts, width), F32),
            pltpu.VMEM((3, n, own_experts, own_hidden, width), BF16),
            pltpu.VMEM((experts, width), BF16),
            pltpu.VMEM((1, lanes), F32),
            pltpu.VMEM((n, 1, lanes), F32),
            pltpu.SemaphoreType.DMA((4,)),
            pltpu.SemaphoreType.DMA((3, rows - 1)),
            pltpu.SemaphoreType.DMA((3, rows - 1)),
            pltpu.SemaphoreType.DMA((rows - 1,)),
            pltpu.SemaphoreType.DMA((rows - 1,)),
            pltpu.SemaphoreType.DMA((5,)),
            pltpu.SemaphoreType.DMA((5,)),
        ],
        compiler_params=pltpu.CompilerParams(collective_id=0, has_side_effects=True),
    )(rep_w1, rep_w3, rep_w2, rep_gate)


def solution(mesh):
    weights = P("row", None, None, "sa")
    return jax.shard_map(
        functools.partial(local, rows=mesh.shape["row"], n=mesh.shape["sa"]),
        mesh=mesh,
        in_specs=(weights, weights, weights, P("row", None, "sa")),
        out_specs=(
            P("row", "sa", None),
            P("row", "sa", None),
            P("row", "sa", None),
            P(),
            P("row", None),
            P("row", None, None),
        ),
        check_vma=False,
    )
```

```python
import functools

import jax
import jax.numpy as jnp
from jax import lax
from jax.experimental import pallas as pl
from jax.experimental.pallas import tpu as pltpu
from jax.sharding import PartitionSpec as P

MESH = pl.DeviceIdType.MESH
F32 = jnp.float32
BF16 = jnp.bfloat16
VMEM_LIMIT = 40 * 1024 * 1024


def scaled(total, replicas):
    if replicas & (replicas - 1) == 0:
        return total * (1.0 / replicas)
    return total / replicas


def square_sum(values):
    squares = values * values
    while squares.ndim > 2:
        squares = jnp.sum(squares, axis=0)
    rows = jnp.sum(squares, axis=0, keepdims=True)
    return jnp.sum(rows, axis=1, keepdims=True)


def kernel(
    rows, n, replicas, counts,
    w1_hbm, w3_hbm, w2_hbm, gate_hbm,
    out1, out3, out2, gate_out, soup_out, rep_out,
    w_in, gate_in, part, part_got, gate_slots, block, gate_block, stats_send, stats_slots,
    in_sem, row_send, row_recv, gate_row_send, gate_row_recv, sa_send, sa_recv,
):
    sources = (w1_hbm, w3_hbm, w2_hbm)
    outs = (out1, out3, out2)
    held, experts, hidden, width = w1_hbm.shape
    own_experts = experts // rows
    own_hidden = hidden // n
    row = lax.axis_index("row")
    me = lax.axis_index("sa")

    loads = [pltpu.make_async_copy(gate_hbm, gate_in, in_sem.at[3])]
    loads += [pltpu.make_async_copy(sources[t], w_in.at[t], in_sem.at[t]) for t in range(3)]
    for load in loads:
        load.start()

    barrier = pltpu.get_barrier_semaphore()

    def greet(step, carry):
        pl.semaphore_signal(
            barrier, inc=1, device_id={"sa": lax.rem(me + step, n)}, device_id_type=MESH
        )
        return carry

    for step in range(1, rows):
        pl.semaphore_signal(
            barrier, inc=1, device_id={"row": lax.rem(row + step, rows)}, device_id_type=MESH
        )
    lax.fori_loop(1, n, greet, 0)

    lane = lax.broadcasted_iota(jnp.int32, (1, stats_send.shape[1]), 1)
    stats = jnp.zeros((1, stats_send.shape[1]), F32)
    soup_lanes = 4 * own_experts

    def rep_lane(replica, expert, t):
        return soup_lanes + 4 * (replica * experts + expert) + t

    loads[0].wait()
    gate_sum = gate_in[0]
    for replica in range(1, held):
        gate_sum = gate_sum + gate_in[replica]
    gate_slots[row] = gate_sum
    for t in range(3):
        loads[1 + t].wait()
        for step in range(1, rows):
            first = lax.rem(row + step, rows) * own_experts
            total = w_in[t, 0, pl.ds(first, own_experts)]
            for replica in range(1, held):
                total = total + w_in[t, replica, pl.ds(first, own_experts)]
            part[t, step - 1] = total

    pl.semaphore_wait(barrier, rows - 1 + n - 1)

    gate_copies = []
    part_copies = []
    for step in range(1, rows):
        gate_copies.append(
            pltpu.make_async_remote_copy(
                src_ref=gate_slots.at[row],
                dst_ref=gate_slots.at[row],
                send_sem=gate_row_send.at[step - 1],
                recv_sem=gate_row_recv.at[step - 1],
                device_id={"row": lax.rem(row + step, rows)},
                device_id_type=MESH,
            )
        )
        gate_copies[-1].start()
    for t in range(3):
        for step in range(1, rows):
            part_copies.append(
                pltpu.make_async_remote_copy(
                    src_ref=part.at[t, step - 1],
                    dst_ref=part_got.at[t, step - 1],
                    send_sem=row_send.at[t, step - 1],
                    recv_sem=row_recv.at[t, step - 1],
                    device_id={"row": lax.rem(row + step, rows)},
                    device_id_type=MESH,
                )
            )
            part_copies[-1].start()

    for replica in range(held):
        for expert in range(experts):
            for t in range(3):
                stats = jnp.where(
                    lane == rep_lane(replica, expert, t),
                    square_sum(w_in[t, replica, expert]),
                    stats,
                )
            stats = jnp.where(
                lane == rep_lane(replica, expert, 3),
                square_sum(gate_in[replica, pl.ds(expert, 1)]),
                stats,
            )

    columns = pl.ds(pl.multiple_of(me * width, width), width)
    own_first = row * own_experts

    for copy in gate_copies:
        copy.wait_recv()
    gate_total = gate_slots[0]
    for other in range(1, rows):
        gate_total = gate_total + gate_slots[other]
    served_gate = scaled(gate_total, replicas).astype(BF16)
    gate_block[...] = served_gate
    gate_out[:, columns] = served_gate

    def send_gate(step, carry):
        pltpu.make_async_remote_copy(
            src_ref=gate_block,
            dst_ref=gate_out.at[:, columns],
            send_sem=sa_send.at[3],
            recv_sem=sa_recv.at[3],
            device_id={"sa": lax.rem(me + step, n)},
            device_id_type=MESH,
        ).start()
        return carry

    lax.fori_loop(1, n, send_gate, 0)

    gate_wide = served_gate.astype(F32)
    gate_squares = jnp.sum(gate_wide * gate_wide, axis=1, keepdims=True)
    expert_row = lax.broadcasted_iota(jnp.int32, gate_squares.shape, 0)
    for own in range(own_experts):
        square = jnp.sum(
            jnp.where(expert_row == own_first + own, gate_squares, 0.0), axis=0, keepdims=True
        )
        stats = jnp.where(lane == 4 * own + 3, square, stats)

    for t in range(3):
        for copy in part_copies[t * (rows - 1):(t + 1) * (rows - 1)]:
            copy.wait_recv()
        total = w_in[t, 0, pl.ds(own_first, own_experts)]
        for replica in range(1, held):
            total = total + w_in[t, replica, pl.ds(own_first, own_experts)]
        for step in range(1, rows):
            total = total + part_got[t, step - 1]
        served = scaled(total, replicas).astype(BF16)
        for dest in range(n):
            block[t, dest] = served[:, dest * own_hidden:(dest + 1) * own_hidden]

        def send_block(step, carry, t=t):
            peer = lax.rem(me + step, n)
            pltpu.make_async_remote_copy(
                src_ref=block.at[t, peer],
                dst_ref=outs[t].at[:, :, columns],
                send_sem=sa_send.at[t],
                recv_sem=sa_recv.at[t],
                device_id={"sa": peer},
                device_id_type=MESH,
            ).start()
            return carry

        lax.fori_loop(1, n, send_block, 0)
        outs[t][:, :, columns] = block[t, me]
        for own in range(own_experts):
            stats = jnp.where(
                lane == 4 * own + t, square_sum(served[own].astype(F32)), stats
            )

    stats_send[...] = stats
    stats_slots[me] = stats

    def send_stats(step, carry):
        pltpu.make_async_remote_copy(
            src_ref=stats_send,
            dst_ref=stats_slots.at[me],
            send_sem=sa_send.at[4],
            recv_sem=sa_recv.at[4],
            device_id={"sa": lax.rem(me + step, n)},
            device_id_type=MESH,
        ).start()
        return carry

    lax.fori_loop(1, n, send_stats, 0)

    others = pl.ds(0, (n - 1) * width)
    landed = [outs[t].at[:, :, others] for t in range(3)]
    landed += [gate_out.at[:, others], stats_slots.at[pl.ds(0, n - 1)]]
    pltpu.make_async_copy(landed[4], landed[4], sa_recv.at[4]).wait()
    norms = stats_slots[0]
    for source in range(1, n):
        norms = norms + stats_slots[source]
    norms = jnp.sqrt(jnp.where(lane % 4 == 3, norms / counts[1], norms / counts[0]))
    for own in range(own_experts):
        soup_out[pl.ds(own, 1), :] = norms[:, 4 * own:4 * own + 4]
    for replica in range(held):
        for expert in range(experts):
            at = rep_lane(replica, expert, 0)
            rep_out[replica, pl.ds(expert, 1), :] = norms[:, at:at + 4]

    for t in (3, 0, 1, 2):
        pltpu.make_async_copy(landed[t], landed[t], sa_recv.at[t]).wait()
    for copy in gate_copies + part_copies:
        copy.wait_send()
    for t in range(5):
        pltpu.make_async_copy(landed[t], landed[t], sa_send.at[t]).wait()


def finish_kernel(*refs):
    count = (len(refs) - 1) // 2
    copies = [
        pltpu.make_async_copy(refs[i], refs[count + i], refs[-1].at[i]) for i in range(count)
    ]
    for copy in copies:
        copy.start()
    for copy in copies:
        copy.wait()


def finish(results):
    return pl.pallas_call(
        finish_kernel,
        out_shape=tuple(jax.ShapeDtypeStruct(r.shape, r.dtype) for r in results),
        in_specs=[pl.BlockSpec(memory_space=pltpu.VMEM)] * len(results),
        out_specs=(pl.BlockSpec(memory_space=pltpu.HBM),) * len(results),
        scratch_shapes=[pltpu.SemaphoreType.DMA((len(results),))],
        compiler_params=pltpu.CompilerParams(vmem_limit_bytes=VMEM_LIMIT),
    )(*results)


def local(rep_w1, rep_w3, rep_w2, rep_gate, rows, n):
    held, experts, hidden, width = rep_w1.shape
    own_experts, own_hidden = experts // rows, hidden // n
    lanes = -(-4 * (own_experts + held * experts) // 128) * 128
    vmem = pl.BlockSpec(memory_space=pltpu.VMEM)
    served = pltpu.VMEM((own_experts, own_hidden, n * width), BF16)
    results = pl.pallas_call(
        functools.partial(
            kernel, rows, n, held * rows, (float(hidden * width * n), float(width * n))
        ),
        out_shape=(
            served,
            served,
            served,
            pltpu.VMEM((experts, n * width), BF16),
            pltpu.VMEM((own_experts, 4), F32),
            pltpu.VMEM((held, experts, 4), F32),
        ),
        in_specs=[pl.BlockSpec(memory_space=pltpu.HBM)] * 4,
        out_specs=(vmem,) * 6,
        scratch_shapes=[
            pltpu.VMEM((3, held, experts, hidden, width), F32),
            pltpu.VMEM((held, experts, width), F32),
            pltpu.VMEM((3, rows - 1, own_experts, hidden, width), F32),
            pltpu.VMEM((3, rows - 1, own_experts, hidden, width), F32),
            pltpu.VMEM((rows, experts, width), F32),
            pltpu.VMEM((3, n, own_experts, own_hidden, width), BF16),
            pltpu.VMEM((experts, width), BF16),
            pltpu.VMEM((1, lanes), F32),
            pltpu.VMEM((n, 1, lanes), F32),
            pltpu.SemaphoreType.DMA((4,)),
            pltpu.SemaphoreType.DMA((3, rows - 1)),
            pltpu.SemaphoreType.DMA((3, rows - 1)),
            pltpu.SemaphoreType.DMA((rows - 1,)),
            pltpu.SemaphoreType.DMA((rows - 1,)),
            pltpu.SemaphoreType.DMA((5,)),
            pltpu.SemaphoreType.DMA((5,)),
        ],
        compiler_params=pltpu.CompilerParams(
            collective_id=0, has_side_effects=True, vmem_limit_bytes=VMEM_LIMIT
        ),
    )(rep_w1, rep_w3, rep_w2, rep_gate)
    return finish(results)


def solution(mesh):
    weights = P("row", None, None, "sa")
    return jax.shard_map(
        functools.partial(local, rows=mesh.shape["row"], n=mesh.shape["sa"]),
        mesh=mesh,
        in_specs=(weights, weights, weights, P("row", None, "sa")),
        out_specs=(
            P("row", "sa", None),
            P("row", "sa", None),
            P("row", "sa", None),
            P(),
            P("row", None),
            P("row", None, None),
        ),
        check_vma=False,
    )
```

```python
import functools

import jax
import jax.numpy as jnp
from jax import lax
from jax.experimental import pallas as pl
from jax.experimental.pallas import tpu as pltpu
from jax.sharding import PartitionSpec as P

MESH = pl.DeviceIdType.MESH
F32 = jnp.float32
BF16 = jnp.bfloat16
VMEM_LIMIT = 16 * 1024 * 1024


def scaled(total, replicas):
    if replicas & (replicas - 1) == 0:
        return total * (1.0 / replicas)
    return total / replicas


def square_sum(values):
    squares = values * values
    while squares.ndim > 2:
        squares = jnp.sum(squares, axis=0)
    rows = jnp.sum(squares, axis=0, keepdims=True)
    return jnp.sum(rows, axis=1, keepdims=True)


def kernel(
    rows, n, replicas, counts,
    w1_hbm, w3_hbm, w2_hbm, gate_hbm,
    out1, out3, out2, gate_out, soup_out, rep_out,
    w_in, gate_in, part, part_got, gate_slots, block, gate_block, stats_send, stats_slots,
    in_sem, row_send, row_recv, gate_row_send, gate_row_recv, sa_send, sa_recv,
):
    sources = (w1_hbm, w3_hbm, w2_hbm)
    outs = (out1, out3, out2)
    held, experts, hidden, width = w1_hbm.shape
    own_experts = experts // rows
    own_hidden = hidden // n
    row = lax.axis_index("row")
    me = lax.axis_index("sa")

    loads = [pltpu.make_async_copy(gate_hbm, gate_in, in_sem.at[3])]
    loads += [pltpu.make_async_copy(sources[t], w_in.at[t], in_sem.at[t]) for t in range(3)]
    for load in loads:
        load.start()

    barrier = pltpu.get_barrier_semaphore()

    def greet(step, carry):
        pl.semaphore_signal(
            barrier, inc=1, device_id={"sa": lax.rem(me + step, n)}, device_id_type=MESH
        )
        return carry

    for step in range(1, rows):
        pl.semaphore_signal(
            barrier, inc=1, device_id={"row": lax.rem(row + step, rows)}, device_id_type=MESH
        )
    lax.fori_loop(1, n, greet, 0)

    lane = lax.broadcasted_iota(jnp.int32, (1, stats_send.shape[1]), 1)
    stats = jnp.zeros((1, stats_send.shape[1]), F32)
    soup_lanes = 4 * own_experts

    def rep_lane(replica, expert, t):
        return soup_lanes + 4 * (replica * experts + expert) + t

    loads[0].wait()
    gate_sum = gate_in[0]
    for replica in range(1, held):
        gate_sum = gate_sum + gate_in[replica]
    gate_slots[row] = gate_sum
    for t in range(3):
        loads[1 + t].wait()
        for step in range(1, rows):
            first = lax.rem(row + step, rows) * own_experts
            total = w_in[t, 0, pl.ds(first, own_experts)]
            for replica in range(1, held):
                total = total + w_in[t, replica, pl.ds(first, own_experts)]
            part[t, step - 1] = total

    pl.semaphore_wait(barrier, rows - 1 + n - 1)

    gate_copies = []
    part_copies = []
    for step in range(1, rows):
        gate_copies.append(
            pltpu.make_async_remote_copy(
                src_ref=gate_slots.at[row],
                dst_ref=gate_slots.at[row],
                send_sem=gate_row_send.at[step - 1],
                recv_sem=gate_row_recv.at[step - 1],
                device_id={"row": lax.rem(row + step, rows)},
                device_id_type=MESH,
            )
        )
        gate_copies[-1].start()
    for t in range(3):
        for step in range(1, rows):
            part_copies.append(
                pltpu.make_async_remote_copy(
                    src_ref=part.at[t, step - 1],
                    dst_ref=part_got.at[t, step - 1],
                    send_sem=row_send.at[t, step - 1],
                    recv_sem=row_recv.at[t, step - 1],
                    device_id={"row": lax.rem(row + step, rows)},
                    device_id_type=MESH,
                )
            )
            part_copies[-1].start()

    for replica in range(held):
        for expert in range(experts):
            for t in range(3):
                stats = jnp.where(
                    lane == rep_lane(replica, expert, t),
                    square_sum(w_in[t, replica, expert]),
                    stats,
                )
            stats = jnp.where(
                lane == rep_lane(replica, expert, 3),
                square_sum(gate_in[replica, pl.ds(expert, 1)]),
                stats,
            )

    columns = pl.ds(pl.multiple_of(me * width, width), width)
    own_first = row * own_experts

    for copy in gate_copies:
        copy.wait_recv()
    gate_total = gate_slots[0]
    for other in range(1, rows):
        gate_total = gate_total + gate_slots[other]
    served_gate = scaled(gate_total, replicas).astype(BF16)
    gate_block[...] = served_gate
    gate_out[:, columns] = served_gate

    def send_gate(step, carry):
        pltpu.make_async_remote_copy(
            src_ref=gate_block,
            dst_ref=gate_out.at[:, columns],
            send_sem=sa_send.at[3],
            recv_sem=sa_recv.at[3],
            device_id={"sa": lax.rem(me + step, n)},
            device_id_type=MESH,
        ).start()
        return carry

    lax.fori_loop(1, n, send_gate, 0)

    gate_wide = served_gate.astype(F32)
    gate_squares = jnp.sum(gate_wide * gate_wide, axis=1, keepdims=True)
    expert_row = lax.broadcasted_iota(jnp.int32, gate_squares.shape, 0)
    for own in range(own_experts):
        square = jnp.sum(
            jnp.where(expert_row == own_first + own, gate_squares, 0.0), axis=0, keepdims=True
        )
        stats = jnp.where(lane == 4 * own + 3, square, stats)

    for t in range(3):
        for copy in part_copies[t * (rows - 1):(t + 1) * (rows - 1)]:
            copy.wait_recv()
        total = w_in[t, 0, pl.ds(own_first, own_experts)]
        for replica in range(1, held):
            total = total + w_in[t, replica, pl.ds(own_first, own_experts)]
        for step in range(1, rows):
            total = total + part_got[t, step - 1]
        served = scaled(total, replicas).astype(BF16)
        for dest in range(n):
            block[t, dest] = served[:, dest * own_hidden:(dest + 1) * own_hidden]

        def send_block(step, carry, t=t):
            peer = lax.rem(me + step, n)
            pltpu.make_async_remote_copy(
                src_ref=block.at[t, peer],
                dst_ref=outs[t].at[:, :, columns],
                send_sem=sa_send.at[t],
                recv_sem=sa_recv.at[t],
                device_id={"sa": peer},
                device_id_type=MESH,
            ).start()
            return carry

        lax.fori_loop(1, n, send_block, 0)
        outs[t][:, :, columns] = block[t, me]
        for own in range(own_experts):
            stats = jnp.where(
                lane == 4 * own + t, square_sum(served[own].astype(F32)), stats
            )

    stats_send[...] = stats
    stats_slots[me] = stats

    def send_stats(step, carry):
        pltpu.make_async_remote_copy(
            src_ref=stats_send,
            dst_ref=stats_slots.at[me],
            send_sem=sa_send.at[4],
            recv_sem=sa_recv.at[4],
            device_id={"sa": lax.rem(me + step, n)},
            device_id_type=MESH,
        ).start()
        return carry

    lax.fori_loop(1, n, send_stats, 0)

    others = pl.ds(0, (n - 1) * width)
    landed = [outs[t].at[:, :, others] for t in range(3)]
    landed += [gate_out.at[:, others], stats_slots.at[pl.ds(0, n - 1)]]
    pltpu.make_async_copy(landed[4], landed[4], sa_recv.at[4]).wait()
    norms = stats_slots[0]
    for source in range(1, n):
        norms = norms + stats_slots[source]
    norms = jnp.sqrt(jnp.where(lane % 4 == 3, norms / counts[1], norms / counts[0]))
    for own in range(own_experts):
        soup_out[pl.ds(own, 1), :] = norms[:, 4 * own:4 * own + 4]
    for replica in range(held):
        for expert in range(experts):
            at = rep_lane(replica, expert, 0)
            rep_out[replica, pl.ds(expert, 1), :] = norms[:, at:at + 4]

    for t in (3, 0, 1, 2):
        pltpu.make_async_copy(landed[t], landed[t], sa_recv.at[t]).wait()
    for copy in gate_copies + part_copies:
        copy.wait_send()
    for t in range(5):
        pltpu.make_async_copy(landed[t], landed[t], sa_send.at[t]).wait()


def finish_kernel(*refs):
    count = (len(refs) - 1) // 2
    copies = [
        pltpu.make_async_copy(refs[i], refs[count + i], refs[-1].at[i]) for i in range(count)
    ]
    for copy in copies:
        copy.start()
    for copy in copies:
        copy.wait()


def finish(results):
    return pl.pallas_call(
        finish_kernel,
        out_shape=tuple(jax.ShapeDtypeStruct(r.shape, r.dtype) for r in results),
        in_specs=[pl.BlockSpec(memory_space=pltpu.VMEM)] * len(results),
        out_specs=(pl.BlockSpec(memory_space=pltpu.HBM),) * len(results),
        scratch_shapes=[pltpu.SemaphoreType.DMA((len(results),))],
        compiler_params=pltpu.CompilerParams(vmem_limit_bytes=VMEM_LIMIT),
    )(*results)


def local(rep_w1, rep_w3, rep_w2, rep_gate, rows, n):
    held, experts, hidden, width = rep_w1.shape
    own_experts, own_hidden = experts // rows, hidden // n
    lanes = -(-4 * (own_experts + held * experts) // 128) * 128
    vmem = pl.BlockSpec(memory_space=pltpu.VMEM)
    served = pltpu.VMEM((own_experts, own_hidden, n * width), BF16)
    results = pl.pallas_call(
        functools.partial(
            kernel, rows, n, held * rows, (float(hidden * width * n), float(width * n))
        ),
        out_shape=(
            served,
            served,
            served,
            pltpu.VMEM((experts, n * width), BF16),
            pltpu.VMEM((own_experts, 4), F32),
            pltpu.VMEM((held, experts, 4), F32),
        ),
        in_specs=[pl.BlockSpec(memory_space=pltpu.HBM)] * 4,
        out_specs=(vmem,) * 6,
        scratch_shapes=[
            pltpu.VMEM((3, held, experts, hidden, width), F32),
            pltpu.VMEM((held, experts, width), F32),
            pltpu.VMEM((3, rows - 1, own_experts, hidden, width), F32),
            pltpu.VMEM((3, rows - 1, own_experts, hidden, width), F32),
            pltpu.VMEM((rows, experts, width), F32),
            pltpu.VMEM((3, n, own_experts, own_hidden, width), BF16),
            pltpu.VMEM((experts, width), BF16),
            pltpu.VMEM((1, lanes), F32),
            pltpu.VMEM((n, 1, lanes), F32),
            pltpu.SemaphoreType.DMA((4,)),
            pltpu.SemaphoreType.DMA((3, rows - 1)),
            pltpu.SemaphoreType.DMA((3, rows - 1)),
            pltpu.SemaphoreType.DMA((rows - 1,)),
            pltpu.SemaphoreType.DMA((rows - 1,)),
            pltpu.SemaphoreType.DMA((5,)),
            pltpu.SemaphoreType.DMA((5,)),
        ],
        compiler_params=pltpu.CompilerParams(
            collective_id=0, has_side_effects=True
        ),
    )(rep_w1, rep_w3, rep_w2, rep_gate)
    return finish(results)


def solution(mesh):
    weights = P("row", None, None, "sa")
    return jax.shard_map(
        functools.partial(local, rows=mesh.shape["row"], n=mesh.shape["sa"]),
        mesh=mesh,
        in_specs=(weights, weights, weights, P("row", None, "sa")),
        out_specs=(
            P("row", "sa", None),
            P("row", "sa", None),
            P("row", "sa", None),
            P(),
            P("row", None),
            P("row", None, None),
        ),
        check_vma=False,
    )
```
